32 devices in a mesh: dp: 16 (over z, y, x), rep: 2 (over core).
Axes of the slice: x: 2, y: 2, z: 4, core: 2. Of those that a mesh axis runs over, the one named last changes fastest.
Arguments:
- pooled: bfloat16 [16, 128, 8192], P(None, ('dp', 'rep')), may hold values from -6 to 6
- slot_of_block: int32 [128], replicated, may hold values from 0 to 127, each once
- dense_part: bfloat16 [128, 8192], P(None, ('dp', 'rep')), may hold values from -6 to 6
- labels: int32 [8192], P(('dp', 'rep')), may hold values 0 or 1
- sample_weight: float32 [8192], P(('dp', 'rep')), may hold values from 0.5 to 18, as said below
- proj_wide: bfloat16 [6, 256, 128], replicated, may hold values from -0.375 to 0.375
- proj_mid: bfloat16 [4, 64, 128], replicated, may hold values from -0.75 to 0.75
- proj_narrow: bfloat16 [16, 16, 128], replicated, may hold values from -1.5 to 1.5
- cross_in: bfloat16 [2, 3456, 256], replicated, may hold values from -0.109375 to 0.109375
- cross_out: bfloat16 [2, 256, 3456], replicated, may hold values from -0.375 to 0.375
- cross_bias: float32 [2, 3456], replicated, may hold values from -3 to 3
- head_weight: float32 [3456], replicated, may hold values from -0.24 to 0.24
Outputs:
- pooled_grad: float32 [16, 128, 8192], P(None, ('dp', 'rep'))
- grad_cross_in: float32 [2, 3456, 256], P(None, ('dp', 'rep'))
- grad_cross_out: float32 [2, 256, 3456], P(None, None, ('dp', 'rep'))
- grad_bias: float32 [2, 3456], P(None, ('dp', 'rep'))
The draws below stay inside these ranges and needn't reach their ends.
Inputs may be any that keep to these rules, and one draw needn't show every extreme that they name: `slot_of_block`: each number of 0 to 127 appears once. `sample_weight`: positive.
All inputs are finite; a program needn't handle non-finite values. No bound on the sum of `labels` on one device may be relied on, other than what follows from the above.
Results may differ from the reference program's by a relative error of at most 0.014.
Values may be sent and summed in bfloat16 or wider, within the bound.
No kernel may reach another device: no remote copies, remote signals or barrier semaphores. Data moves between devices by JAX's collectives and lax.ppermute only.
A program may use at most 128 MiB of HBM per device.

```python
import math
import jax
import jax.numpy as jnp
from jax import lax

BLOCK_WIDTH = 16
WIDE_TABLES = 6
MID_TABLES = 4
NARROW_TABLES = 16
WIDE_WIDTH = 256
MID_WIDTH = 64
NARROW_WIDTH = 16
PROJECTED = 128
CROSS_RANK = 256
LAYERS = 2
ROWS_DEV = 256
BLOCKS = 128
CROSS_WIDTH = 3456
BATCH_ROWS = 8192
N_DP = 16
N_REP = 2


def draw_sample_weight(key, part):
    base_weight = jnp.exp(jax.random.uniform(key, (BATCH_ROWS,), jnp.float32, math.log(0.5), math.log(2.0)))
    owner_index = (jnp.arange(BATCH_ROWS) // ROWS_DEV).astype(jnp.float32)
    fraction = owner_index / max(N_DP * N_REP - 1, 1)
    factor = 1.0 + 2.0 * fraction
    return (base_weight * factor).astype(jnp.float32)


def place_ends(entries, key, smallest, high):
    place = [jax.random.randint(jax.random.fold_in(key, axis), (), 0, length) for axis, length in enumerate(entries.shape)]
    main_axis = entries.shape.index(max(entries.shape))
    next_to = place[:main_axis] + [(place[main_axis] + 1) % entries.shape[main_axis]] + place[main_axis + 1:]
    return entries.at[tuple(place)].set(smallest).at[tuple(next_to)].set(high)


def shard_levels(own_key, shape, cuts, low, high):
    factor_of = 1.0
    for axis_at, blocks in cuts:
        heights = jax.random.uniform(jax.random.fold_in(jax.random.fold_in(own_key, 6), axis_at), (blocks,), jnp.float32, low / len(cuts), high / len(cuts))
        factor_of = factor_of * jnp.repeat(jnp.exp(heights), shape[axis_at] // blocks).reshape((-1,) + (1,) * (len(shape) - 1 - axis_at))
    return factor_of


def scatter_about(key, shape, deviation, reach, cuts=(), kind=jnp.bfloat16):
    array = deviation * jax.random.normal(key, shape, jnp.float32)
    if cuts:
        array = array * shard_levels(key, shape, cuts, -0.22, 0.18)
    return jnp.clip(array, -reach, reach).astype(kind)


def setup_inputs(seed: int = 0) -> dict:
    key_list = jax.random.split(jax.random.key(seed), 13)
    return {
        "pooled": scatter_about(key_list[0], (BLOCK_WIDTH, BLOCKS, BATCH_ROWS), 1.0, 6.0, ((1, 32),)),
        "slot_of_block": jax.random.permutation(key_list[1], BLOCKS).astype(jnp.int32),
        "dense_part": scatter_about(key_list[2], (PROJECTED, BATCH_ROWS), 1.0, 6.0, ((1, 32),)),
        "labels": place_ends((jax.random.randint(key_list[3], (BATCH_ROWS,), 0, 2) < 1).astype(jnp.int32), jax.random.fold_in(key_list[3], 1), 0, 1),
        "sample_weight": draw_sample_weight(jax.random.fold_in(key_list[12], 71), 0),
        "proj_wide": scatter_about(key_list[5], (WIDE_TABLES, WIDE_WIDTH, PROJECTED), WIDE_WIDTH ** -0.5, 0.375),
        "proj_mid": scatter_about(key_list[6], (MID_TABLES, MID_WIDTH, PROJECTED), MID_WIDTH ** -0.5, 0.75),
        "proj_narrow": scatter_about(key_list[7], (NARROW_TABLES, NARROW_WIDTH, PROJECTED), NARROW_WIDTH ** -0.5, 1.5),
        "cross_in": scatter_about(key_list[8], (LAYERS, CROSS_WIDTH, CROSS_RANK), CROSS_WIDTH ** -0.5, 0.109375),
        "cross_out": scatter_about(key_list[9], (LAYERS, CROSS_RANK, CROSS_WIDTH), CROSS_RANK ** -0.5, 0.375),
        "cross_bias": scatter_about(key_list[10], (LAYERS, CROSS_WIDTH), 0.5, 3.0, (), jnp.float32),
        "head_weight": scatter_about(key_list[11], (CROSS_WIDTH,), 0.04, 0.24, (), jnp.float32),
    }


def table_layout():
    first_end = WIDE_TABLES * (WIDE_WIDTH // BLOCK_WIDTH)
    second_end = first_end + MID_TABLES * (MID_WIDTH // BLOCK_WIDTH)
    return ((0, first_end, WIDE_TABLES, WIDE_WIDTH), (first_end, second_end, MID_TABLES, MID_WIDTH), (second_end, BLOCKS, NARROW_TABLES, NARROW_WIDTH))


def project_tables(logical, proj_tables):
    row_count = logical.shape[2]
    outputs = []
    for layout, proj_table in zip(table_layout(), proj_tables):
        block_start, block_end, table_count, table_width = layout
        pieces = logical[:, block_start:block_end].reshape(BLOCK_WIDTH, table_count, table_width // BLOCK_WIDTH, row_count)
        matrix = proj_table.reshape(table_count, table_width // BLOCK_WIDTH, BLOCK_WIDTH, PROJECTED)
        result = jnp.einsum('tkco,ctkr->tor', matrix.astype(jnp.float32), pieces.astype(jnp.float32))
        outputs.append(result.reshape(table_count * PROJECTED, row_count))
    return jnp.concatenate(outputs, 0)


def project_back(proj_grad, proj_tables):
    row_count = proj_grad.shape[1]
    outputs = []
    offset = 0
    for layout, proj_table in zip(table_layout(), proj_tables):
        block_start, block_end, table_count, table_width = layout
        piece = proj_grad[offset:offset + table_count * PROJECTED].reshape(table_count, PROJECTED, row_count)
        offset = offset + table_count * PROJECTED
        matrix = proj_table.reshape(table_count, table_width // BLOCK_WIDTH, BLOCK_WIDTH, PROJECTED)
        result = jnp.einsum('tkco,tor->ctkr', matrix.astype(jnp.float32), piece.astype(jnp.float32))
        outputs.append(result.reshape(BLOCK_WIDTH, block_end - block_start, row_count))
    return jnp.concatenate(outputs, 1)


def block_step(slots, dense_part, labels, sample_weight, slot_of_block, proj_tables, cross_in, cross_out, cross_bias, head_weight):
    logical = jnp.take(slots, slot_of_block, axis=1)
    projected = project_tables(logical, proj_tables)
    start = jnp.concatenate([dense_part.astype(jnp.float32), projected], 0).astype(jnp.bfloat16)
    start_full = start.astype(jnp.float32)
    layer_inputs = [start]
    hidden_list = []
    gate_list = []
    current = start
    for layer in range(LAYERS):
        hidden = jnp.dot(cross_in[layer].T, current, preferred_element_type=jnp.float32).astype(jnp.bfloat16)
        gate = jnp.dot(cross_out[layer].T, hidden, preferred_element_type=jnp.float32) + cross_bias[layer][:, None]
        current = (start_full * gate + current.astype(jnp.float32)).astype(jnp.bfloat16)
        hidden_list.append(hidden)
        gate_list.append(gate)
        layer_inputs.append(current)
    logit = jnp.dot(head_weight, current.astype(jnp.float32), precision=lax.Precision.HIGHEST)
    signal = sample_weight * (jax.nn.sigmoid(logit) - labels.astype(jnp.float32))
    upstream = head_weight[:, None] * signal[None, :]
    start_grad = jnp.zeros(start_full.shape, jnp.float32)
    in_terms = [None] * LAYERS
    out_terms = [None] * LAYERS
    bias_terms = [None] * LAYERS
    for layer in reversed(range(LAYERS)):
        gate_grad = start_full * upstream
        bias_terms[layer] = jnp.sum(gate_grad, axis=1)
        gate_low = gate_grad.astype(jnp.bfloat16)
        out_terms[layer] = jnp.dot(hidden_list[layer], gate_low.T, preferred_element_type=jnp.float32)
        hidden_grad = jnp.dot(cross_out[layer], gate_low, preferred_element_type=jnp.float32).astype(jnp.bfloat16)
        in_terms[layer] = jnp.dot(layer_inputs[layer], hidden_grad.T, preferred_element_type=jnp.float32)
        start_grad = start_grad + gate_list[layer] * upstream
        upstream = upstream + jnp.dot(cross_in[layer], hidden_grad, preferred_element_type=jnp.float32)
    start_grad = start_grad + upstream
    proj_grad = start_grad[PROJECTED:].astype(jnp.bfloat16)
    logical_grad = project_back(proj_grad, proj_tables)
    slot_grad = jnp.zeros(logical_grad.shape, jnp.float32).at[:, slot_of_block, :].set(logical_grad)
    return slot_grad, jnp.stack(in_terms), jnp.stack(out_terms), jnp.stack(bias_terms)


def reference(pooled, slot_of_block, dense_part, labels, sample_weight, proj_wide, proj_mid, proj_narrow, cross_in, cross_out, cross_bias, head_weight):
    total = jnp.sum(sample_weight)
    scale = BATCH_ROWS / total
    proj_tables = (proj_wide, proj_mid, proj_narrow)
    block_count = N_DP * N_REP

    def step(carry, index):
        row_start = (index * ROWS_DEV).astype(jnp.int32)
        slots = lax.dynamic_slice_in_dim(pooled, row_start, ROWS_DEV, 2)
        dense_rows = lax.dynamic_slice_in_dim(dense_part, row_start, ROWS_DEV, 1)
        label_rows = lax.dynamic_slice_in_dim(labels, row_start, ROWS_DEV, 0)
        weight_rows = lax.dynamic_slice_in_dim(sample_weight, row_start, ROWS_DEV, 0)
        slot_grad, in_term, out_term, bias_term = block_step(slots, dense_rows, label_rows, weight_rows, slot_of_block, proj_tables, cross_in, cross_out, cross_bias, head_weight)
        return (carry[0] + in_term, carry[1] + out_term, carry[2] + bias_term), slot_grad

    initial = (jnp.zeros((LAYERS, CROSS_WIDTH, CROSS_RANK), jnp.float32), jnp.zeros((LAYERS, CROSS_RANK, CROSS_WIDTH), jnp.float32), jnp.zeros((LAYERS, CROSS_WIDTH), jnp.float32))
    sums, stacked = lax.scan(step, initial, jnp.arange(block_count, dtype=jnp.int32))
    pooled_grad = jnp.moveaxis(stacked, 0, 2).reshape(BLOCK_WIDTH, BLOCKS, BATCH_ROWS) * scale
    return (pooled_grad, sums[0] * scale, sums[1] * scale, sums[2] * scale)
```

```python
import jax
import jax.numpy as jnp
from jax import lax
from jax.experimental import pallas as pl
from jax.experimental.pallas import tpu as pltpu
from jax.sharding import PartitionSpec as P

BLOCK_WIDTH = 16
PROJECTED = 128
LANES = 128
AXES = ("dp", "rep")
NN = (((1,), (0,)), ((), ()))
NT = (((1,), (1,)), ((), ()))
BF = jnp.bfloat16
F32 = jnp.float32


def dot(a, b, dims=NN):
    return lax.dot_general(a, b, dims, preferred_element_type=F32)


def exchange_basis(dp_count, rep_count):
    bits = dp_count.bit_length() - 1
    low = bits - 2
    masks = []
    if low <= 2:
        masks += [1 << i for i in range(max(low, 0))]
    else:
        for base in range(0, low, 2):
            masks += [1 << base, 3 << base]
    if bits >= 2:
        masks += [1 << low, 2 << low]
    elif bits == 1:
        masks += [1]
    core = [1 << i for i in range(rep_count.bit_length() - 1)]
    return core, [m * rep_count for m in masks]


def basis_digits(index, masks):
    digits = {}
    for mask in sorted(masks, reverse=True):
        top = mask.bit_length() - 1
        bit = (index >> top) & 1
        digits[mask] = bit
        index = index ^ (bit * mask)
    return digits


def position_of(index, order):
    digits = basis_digits(index, order)
    place = 0
    for mask in order:
        place = place * 2 + digits[mask]
    return place


def pack_kernel(weight_ref, x_ref, out_ref, tmp_ref):
    group, depth, lanes = out_ref.shape
    width, blocks, span = x_ref.shape
    per = span // (group * lanes)
    for c in range(width):
        for m in range(group * per):
            tmp_ref[m, pl.ds(c, blocks, stride=width), :] = x_ref[c, :, m * lanes : (m + 1) * lanes].astype(F32)
    total = jnp.sum(jnp.sum(weight_ref[...], 0, keepdims=True), 1, keepdims=True)
    first = total.astype(BF).astype(F32)
    second = (total - first).astype(BF).astype(F32)
    third = total - first - second
    row = lax.broadcasted_iota(jnp.int32, (8, lanes), 0)
    tail = jnp.where(row == 0, first, jnp.where(row == 1, second, jnp.where(row == 2, third, 0.0)))
    for g in range(group):
        for j in range(blocks):
            for h in range(per):
                out_ref[g, (j * per + h) * width : (j * per + h + 1) * width, :] = tmp_ref[
                    g * per + h, j * width : (j + 1) * width, :
                ].astype(BF)
        out_ref[g, depth - 8 : depth, :] = tail.astype(BF)


def pack(pooled, weight, devices):
    width, blocks, batch = pooled.shape
    rows = batch // devices
    per = rows // LANES
    group = 4
    depth = blocks * per * width + 8
    return pl.pallas_call(
        pack_kernel,
        grid=(devices // group,),
        in_specs=[
            pl.BlockSpec((per, LANES), lambda i: (0, 0)),
            pl.BlockSpec((width, blocks, group * rows), lambda i: (0, 0, i)),
        ],
        out_specs=pl.BlockSpec((group, depth, LANES), lambda i: (i, 0, 0)),
        out_shape=jax.ShapeDtypeStruct((devices, depth, LANES), BF),
        scratch_shapes=[pltpu.VMEM((group * per, blocks * width, LANES), F32)],
        name="pack",
    )(weight.reshape(per, LANES), pooled)


def unpack_kernel(x_ref, out_ref, tmp_ref):
    group, _, rows = x_ref.shape
    width, blocks, _ = out_ref.shape
    lanes = tmp_ref.shape[2]
    per = rows // lanes
    for m in range(group * per):
        at = (m % per) * lanes
        tmp_ref[m] = x_ref[m // per, :, at : at + lanes].astype(F32)
        for c in range(width):
            out_ref[c, :, m * lanes : (m + 1) * lanes] = tmp_ref[m, pl.ds(c, blocks, stride=width), :]


def unpack(received):
    width = BLOCK_WIDTH
    devices, both, rows = received.shape
    blocks = both // width
    group = 4
    return pl.pallas_call(
        unpack_kernel,
        grid=(devices // group,),
        in_specs=[pl.BlockSpec((group, both, rows), lambda i: (i, 0, 0))],
        out_specs=pl.BlockSpec((width, blocks, group * rows), lambda i: (0, 0, i)),
        out_shape=jax.ShapeDtypeStruct((width, blocks, devices * rows), F32),
        scratch_shapes=[pltpu.VMEM((group * rows // LANES, both, LANES), F32)],
        name="unpack",
    )(received)


def make_step(tables, devices, blocks_here):
    def kernel(
        slot_ref,
        x_ref,
        dense_ref,
        row_ref,
        col_ref,
        pt0,
        pt1,
        pt2,
        p0,
        p1,
        p2,
        cit_hbm,
        ci_hbm,
        cot_hbm,
        co_hbm,
        back_ref,
        start,
        layer1,
        low1,
        low0,
        small,
        cit_ref,
        ci_ref,
        cot_ref,
        co_ref,
        low,
        gate0,
        gate1,
        sems,
    ):
        pts, ps = (pt0, pt1, pt2), (p0, p1, p2)
        width, rows = start.shape
        tile_rows = 3 * PROJECTED
        tiles = width // tile_rows
        per = rows // LANES

        names = {"cit": (cit_hbm, cit_ref), "cot": (cot_hbm, cot_ref), "co": (co_hbm, co_ref), "ci": (ci_hbm, ci_ref)}
        uses = [("cit", 0), ("cot", 0), ("cit", 1), ("cot", 1), ("co", 1), ("ci", 1), ("co", 0), ("ci", 0)]

        def fetch(n):
            name, layer = uses[n]
            source, target = names[name]
            return pltpu.make_async_copy(source.at[layer], target.at[layer], sems.at[n])

        for n in range(len(uses)):
            fetch(n).start()

        def tile(i):
            return pl.ds(pl.multiple_of(i * tile_rows, tile_rows), tile_rows)

        def loop(body, init=None):
            if init is None:
                lax.fori_loop(0, tiles, lambda i, c: (body(i), c)[1], 0)
                return None
            return lax.fori_loop(0, tiles, body, init)

        start[0:PROJECTED, :] = dense_ref[...]
        for t, (first, count, kind, index) in enumerate(tables):
            parts = []
            for k in range(count):
                slot = slot_ref[first + k]
                at = (slot % blocks_here) * (per * BLOCK_WIDTH)
                pieces = [
                    x_ref[slot // blocks_here, pl.ds(pl.multiple_of(at + h * BLOCK_WIDTH, 16), BLOCK_WIDTH), :]
                    for h in range(per)
                ]
                parts.append(jnp.concatenate(pieces, 1))
            block = parts[0] if count == 1 else jnp.concatenate(parts, 0)
            start[(t + 1) * PROJECTED : (t + 2) * PROJECTED, :] = dot(pts[kind][index], block).astype(BF)

        fetch(0).wait()
        hidden0 = dot(cit_ref[0], start[...]).astype(BF)
        small[0] = hidden0
        fetch(1).wait()

        def fwd0(i):
            s = start[tile(i), :].astype(F32)
            g = dot(cot_ref[0, tile(i), :], hidden0) + col_ref[tile(i), 0:1]
            gate0[tile(i), :] = g
            layer1[tile(i), :] = (s * g + s).astype(BF)

        loop(fwd0)
        fetch(2).wait()
        hidden1 = dot(cit_ref[1], layer1[...]).astype(BF)
        small[1] = hidden1
        fetch(3).wait()

        def fwd1(i, logit):
            s = start[tile(i), :].astype(F32)
            g = dot(cot_ref[1, tile(i), :], hidden1) + col_ref[tile(i), 1:2]
            gate1[tile(i), :] = g
            last = (s * g + layer1[tile(i), :].astype(F32)).astype(BF).astype(F32)
            term = last * col_ref[tile(i), 2:3]
            return logit + jnp.sum(term.reshape(tile_rows // 8, 8, rows), 0)

        partial = loop(fwd1, jnp.zeros((8, rows), F32))
        logit = jnp.sum(partial, 0, keepdims=True)
        depth = x_ref.shape[1]

        def gather_total(d, carry):
            return carry + x_ref[d][depth - 8 : depth, :].astype(F32)

        terms = lax.fori_loop(0, devices, gather_total, jnp.zeros((8, LANES), F32))
        total = jnp.sum(terms, 0, keepdims=True)[:, 0:1]
        scale = float(rows * devices) / total
        signal = scale * row_ref[0:1, :] * (jax.nn.sigmoid(logit) - row_ref[1:2, :])

        def bwd1(i):
            s = start[tile(i), :].astype(F32)
            low1[tile(i), :] = (s * (col_ref[tile(i), 2:3] * signal)).astype(BF)

        loop(bwd1)
        fetch(4).wait()
        hgrad1 = dot(co_ref[1], low1[...]).astype(BF)
        small[2] = hgrad1
        fetch(5).wait()

        def mid(i):
            s = start[tile(i), :].astype(F32)
            up2 = col_ref[tile(i), 2:3] * signal
            up1 = up2 + dot(ci_ref[1, tile(i), :], hgrad1)
            gate1[tile(i), :] = up1 + gate1[tile(i), :] * up2 + gate0[tile(i), :] * up1
            low0[tile(i), :] = (s * up1).astype(BF)

        loop(mid)
        fetch(6).wait()
        hgrad0 = dot(co_ref[0], low0[...]).astype(BF)
        small[3] = hgrad0
        fetch(7).wait()

        def fin(i):
            low[tile(i), :] = (gate1[tile(i), :] + dot(ci_ref[0, tile(i), :], hgrad0)).astype(BF)

        loop(fin)
        for t, (first, count, kind, index) in enumerate(tables):
            grad = low[(t + 1) * PROJECTED : (t + 2) * PROJECTED, :]
            block = dot(ps[kind][index], grad).astype(BF)
            for k in range(count):
                back_ref[slot_ref[first + k]] = block[k * BLOCK_WIDTH : (k + 1) * BLOCK_WIDTH, :]

    return kernel


def make_grads(orders, splits, devices, chunk, chunk_pad):
    half = devices // 2
    colors = len(splits)

    def kernel(me_ref, start, layer1, low1, low0, small, *refs):
        los, his, acc = refs[:colors], refs[colors : 2 * colors], refs[2 * colors]
        group, rows = start.shape
        rank = small.shape[1]
        subs = group // chunk
        me = me_ref[0]
        acc[:, 0:rank] = dot(low1[...], small[1], NT)
        acc[:, rank : 2 * rank] = dot(layer1[...], small[2], NT)
        acc[:, 2 * rank : 3 * rank] = dot(low0[...], small[0], NT)
        acc[:, 3 * rank : 4 * rank] = dot(start[...], small[3], NT)
        ones = jnp.ones((8, rows), BF)
        biases = (dot(ones, low1[...], NT), dot(ones, low0[...], NT))
        spare = chunk_pad - chunk
        for s in range(subs):
            d = pl.program_id(0) * subs + s
            at = 0
            for which, cols in enumerate(splits):
                piece = acc[s * chunk : (s + 1) * chunk, at : at + cols]
                at += cols
                if which < 2:
                    tail = biases[which][0:spare, s * chunk : (s + 1) * chunk]
                    tail = jnp.concatenate([tail, jnp.zeros((spare, cols - chunk), F32)], 1)
                else:
                    tail = jnp.zeros((spare, cols), F32)
                value = jnp.concatenate([piece, tail], 0).astype(BF)
                place = position_of(d ^ me, orders[which])

                @pl.when(place < half)
                def _():
                    los[which][place] = value

                @pl.when(place >= half)
                def _():
                    his[which][place - half] = value

    return kernel


def add_pair(a, b):
    return (a.astype(F32) + b.astype(F32)).astype(BF)


def reduce_pieces(los, his, orders, devices):
    stages = len(orders[0])
    for k in range(stages):
        got = [
            lax.ppermute(h, AXES, [(i, i ^ o[k]) for i in range(devices)])
            for h, o in zip(his, orders)
        ]
        got = lax.optimization_barrier(got)
        if k == stages - 1:
            return [add_pair(a, b)[0] for a, b in zip(los, got)]
        n = los[0].shape[0] // 2
        his = [add_pair(a[n:], b[n:]) for a, b in zip(los, got)]
        los = [add_pair(a[:n], b[:n]) for a, b in zip(los, got)]


def body(
    pooled,
    slot_of_block,
    dense_part,
    labels,
    sample_weight,
    proj_wide,
    proj_mid,
    proj_narrow,
    cross_in,
    cross_out,
    cross_bias,
    head_weight,
):
    dp_count, rep_count = lax.axis_size("dp"), lax.axis_size("rep")
    devices = dp_count * rep_count
    rows = labels.shape[0]
    blocks_here = pooled.shape[1]
    width = cross_bias.shape[1]
    rank = cross_in.shape[2]
    chunk = width // devices
    chunk_pad = (chunk // 8 + 1) * 8

    core, masks = exchange_basis(dp_count, rep_count)
    last = masks[-1:]
    others = masks[:-1]
    colors = 3
    orders = [
        core + [others[(c + i) % len(others)] for i in range(len(others))] + last for c in range(colors)
    ]
    splits = [(4 * rank // LANES + colors - 1 - c) // colors * LANES for c in range(colors)]
    tables = []
    first = 0
    for kind, proj in enumerate((proj_wide, proj_mid, proj_narrow)):
        per = proj.shape[1] // BLOCK_WIDTH
        for index in range(proj.shape[0]):
            tables.append((first, per, kind, index))
            first += per

    received = lax.all_to_all(pack(pooled, sample_weight, devices), AXES, 0, 0, tiled=True)
    row_data = jnp.stack([sample_weight, labels.astype(F32)])
    col_data = jnp.stack([cross_bias[0], cross_bias[1], head_weight], 1)
    me = lax.axis_index(AXES).astype(jnp.int32).reshape(1)

    smem = pl.BlockSpec(memory_space=pltpu.SMEM)
    vmem = pl.BlockSpec(memory_space=pltpu.VMEM)
    hbm = pl.BlockSpec(memory_space=pl.ANY)
    wide = jax.ShapeDtypeStruct((width, rows), BF)
    back, start, layer1, low1, low0, small = pl.pallas_call(
        make_step(tables, devices, blocks_here),
        in_specs=[smem] + [vmem] * 10 + [hbm] * 4,
        out_specs=[vmem] * 6,
        out_shape=[
            jax.ShapeDtypeStruct((blocks_here * devices, BLOCK_WIDTH, rows), BF),
            wide,
            wide,
            wide,
            wide,
            jax.ShapeDtypeStruct((4, rank, rows), BF),
        ],
        scratch_shapes=[
            pltpu.VMEM((2, rank, width), BF),
            pltpu.VMEM((2, width, rank), BF),
            pltpu.VMEM((2, width, rank), BF),
            pltpu.VMEM((2, rank, width), BF),
            pltpu.VMEM((width, rows), BF),
            pltpu.VMEM((width, rows), F32),
            pltpu.VMEM((width, rows), F32),
            pltpu.SemaphoreType.DMA((8,)),
        ],
        compiler_params=pltpu.CompilerParams(vmem_limit_bytes=50 << 20),
        cost_estimate=pl.CostEstimate(flops=16 * width * rank * rows, bytes_accessed=20 << 20, transcendentals=rows),
        name="step",
    )(
        slot_of_block,
        received,
        dense_part,
        row_data,
        col_data,
        jnp.swapaxes(proj_wide, 1, 2),
        jnp.swapaxes(proj_mid, 1, 2),
        jnp.swapaxes(proj_narrow, 1, 2),
        proj_wide,
        proj_mid,
        proj_narrow,
        jnp.swapaxes(cross_in, 1, 2),
        cross_in,
        jnp.swapaxes(cross_out, 1, 2),
        cross_out,
    )
    back = back.reshape(devices, blocks_here * BLOCK_WIDTH, rows)
    back = lax.all_to_all(back, AXES, 0, 0, tiled=True)

    group = chunk
    while group % 16:
        group += chunk
    part = pl.BlockSpec((group, rows), lambda i: (i, 0))
    half = [jax.ShapeDtypeStruct((devices // 2, chunk_pad, c), BF) for c in splits]
    outs = pl.pallas_call(
        make_grads(orders, splits, devices, chunk, chunk_pad),
        grid=(width // group,),
        in_specs=[smem, part, part, part, part, pl.BlockSpec((4, rank, rows), lambda i: (0, 0, 0))],
        out_specs=[pl.BlockSpec(h.shape, lambda i: (0, 0, 0)) for h in half + half],
        out_shape=half + half,
        scratch_shapes=[pltpu.VMEM((group, 4 * rank), F32)],
        compiler_params=pltpu.CompilerParams(vmem_limit_bytes=32 << 20),
        cost_estimate=pl.CostEstimate(flops=8 * width * rank * rows, bytes_accessed=16 << 20, transcendentals=0),
        name="grads",
    )(me, start, layer1, low1, low0, small)
    sums = reduce_pieces(list(outs[:colors]), list(outs[colors:]), orders, devices)
    pooled_grad = unpack(back)
    bias1, bias0 = sums[0][chunk, :chunk], sums[1][chunk, :chunk]
    flat = jnp.concatenate([x[:chunk] for x in sums], 1)
    out1, in1, out0, in0 = [flat[:, i * rank : (i + 1) * rank] for i in range(4)]
    grad_in = jnp.stack([in0, in1]).astype(F32)
    grad_out = jnp.stack([out0.T, out1.T]).astype(F32)
    grad_bias = jnp.stack([bias0, bias1]).astype(F32)
    return (pooled_grad, grad_in, grad_out, grad_bias)


def solution(mesh):
    return jax.shard_map(
        body,
        mesh=mesh,
        in_specs=(
            P(None, AXES, None),
            P(),
            P(None, AXES),
            P(AXES),
            P(AXES),
            P(),
            P(),
            P(),
            P(),
            P(),
            P(),
            P(),
        ),
        out_specs=(
            P(None, AXES, None),
            P(None, AXES, None),
            P(None, None, AXES),
            P(None, AXES),
        ),
        check_vma=False,
    )
```

```python
import jax
import jax.numpy as jnp
from jax import lax
from jax.experimental import pallas as pl
from jax.experimental.pallas import tpu as pltpu
from jax.sharding import PartitionSpec as P

BLOCK_WIDTH = 16
PROJECTED = 128
LANES = 128
AXES = ("dp", "rep")
NN = (((1,), (0,)), ((), ()))
NT = (((1,), (1,)), ((), ()))
BF = jnp.bfloat16
F32 = jnp.float32


def dot(a, b, dims=NN):
    return lax.dot_general(a, b, dims, preferred_element_type=F32)


def exchange_basis(dp_count, rep_count):
    bits = dp_count.bit_length() - 1
    low = bits - 2
    masks = []
    if low <= 2:
        masks += [1 << i for i in range(max(low, 0))]
    else:
        for base in range(0, low, 2):
            masks += [1 << base, 3 << base]
    if bits >= 2:
        masks += [1 << low, 2 << low]
    elif bits == 1:
        masks += [1]
    core = [1 << i for i in range(rep_count.bit_length() - 1)]
    return core, [m * rep_count for m in masks]


def basis_digits(index, masks):
    digits = {}
    for mask in sorted(masks, reverse=True):
        top = mask.bit_length() - 1
        bit = (index >> top) & 1
        digits[mask] = bit
        index = index ^ (bit * mask)
    return digits


def position_of(index, order):
    digits = basis_digits(index, order)
    place = 0
    for mask in order:
        place = place * 2 + digits[mask]
    return place


def pack_kernel(weight_ref, x_ref, out_ref, tmp_ref):
    group, depth, lanes = out_ref.shape
    width, blocks, span = x_ref.shape
    per = span // (group * lanes)
    for c in range(width):
        for m in range(group * per):
            tmp_ref[m, pl.ds(c, blocks, stride=width), :] = x_ref[c, :, m * lanes : (m + 1) * lanes].astype(F32)
    total = jnp.sum(jnp.sum(weight_ref[...], 0, keepdims=True), 1, keepdims=True)
    first = total.astype(BF).astype(F32)
    second = (total - first).astype(BF).astype(F32)
    third = total - first - second
    row = lax.broadcasted_iota(jnp.int32, (8, lanes), 0)
    tail = jnp.where(row == 0, first, jnp.where(row == 1, second, jnp.where(row == 2, third, 0.0)))
    for g in range(group):
        for j in range(blocks):
            for h in range(per):
                out_ref[g, (j * per + h) * width : (j * per + h + 1) * width, :] = tmp_ref[
                    g * per + h, j * width : (j + 1) * width, :
                ].astype(BF)
        out_ref[g, depth - 8 : depth, :] = tail.astype(BF)


def pack(pooled, weight, devices):
    width, blocks, batch = pooled.shape
    rows = batch // devices
    per = rows // LANES
    group = 16
    depth = blocks * per * width + 8
    return pl.pallas_call(
        pack_kernel,
        grid=(devices // group,),
        in_specs=[
            pl.BlockSpec((per, LANES), lambda i: (0, 0)),
            pl.BlockSpec((width, blocks, group * rows), lambda i: (0, 0, i)),
        ],
        out_specs=pl.BlockSpec((group, depth, LANES), lambda i: (i, 0, 0)),
        out_shape=jax.ShapeDtypeStruct((devices, depth, LANES), BF),
        scratch_shapes=[pltpu.VMEM((group * per, blocks * width, LANES), F32)],
        name="pack",
    )(weight.reshape(per, LANES), pooled)


def unpack_kernel(x_ref, out_ref, tmp_ref):
    group, _, rows = x_ref.shape
    width, blocks, _ = out_ref.shape
    lanes = tmp_ref.shape[2]
    per = rows // lanes
    for m in range(group * per):
        at = (m % per) * lanes
        tmp_ref[m] = x_ref[m // per, :, at : at + lanes].astype(F32)
        for c in range(width):
            out_ref[c, :, m * lanes : (m + 1) * lanes] = tmp_ref[m, pl.ds(c, blocks, stride=width), :]


def unpack(received):
    width = BLOCK_WIDTH
    devices, both, rows = received.shape
    blocks = both // width
    group = 8
    return pl.pallas_call(
        unpack_kernel,
        grid=(devices // group,),
        in_specs=[pl.BlockSpec((group, both, rows), lambda i: (i, 0, 0))],
        out_specs=pl.BlockSpec((width, blocks, group * rows), lambda i: (0, 0, i)),
        out_shape=jax.ShapeDtypeStruct((width, blocks, devices * rows), F32),
        scratch_shapes=[pltpu.VMEM((group * rows // LANES, both, LANES), F32)],
        name="unpack",
    )(received)


def make_step(tables, devices, blocks_here):
    def kernel(
        slot_ref,
        x_ref,
        dense_ref,
        row_ref,
        col_ref,
        pt0,
        pt1,
        pt2,
        p0,
        p1,
        p2,
        cit_hbm,
        ci_hbm,
        cot_hbm,
        co_hbm,
        back_ref,
        start_hbm,
        layer1_hbm,
        low1_hbm,
        low0_hbm,
        small,
        start,
        layer1,
        low1,
        low0,
        cit_ref,
        ci_ref,
        cot_ref,
        co_ref,
        low,
        gate0,
        gate1,
        sems,
        out_sems,
    ):
        pts, ps = (pt0, pt1, pt2), (p0, p1, p2)
        width, rows = start.shape
        tile_rows = 3 * PROJECTED
        tiles = width // tile_rows
        per = rows // LANES

        names = {"cit": (cit_hbm, cit_ref), "cot": (cot_hbm, cot_ref), "co": (co_hbm, co_ref), "ci": (ci_hbm, ci_ref)}
        uses = [("cit", 0), ("cot", 0), ("cit", 1), ("cot", 1), ("co", 1), ("ci", 1), ("co", 0), ("ci", 0)]

        def fetch(n):
            name, layer = uses[n]
            source, target = names[name]
            return pltpu.make_async_copy(source.at[layer], target.at[layer], sems.at[n])

        for n in range(len(uses)):
            fetch(n).start()
        written = ((start, start_hbm), (layer1, layer1_hbm), (low1, low1_hbm), (low0, low0_hbm))

        def save(n):
            source, target = written[n]
            return pltpu.make_async_copy(source, target, out_sems.at[n])

        def tile(i):
            return pl.ds(pl.multiple_of(i * tile_rows, tile_rows), tile_rows)

        def loop(body, init=None):
            if init is None:
                lax.fori_loop(0, tiles, lambda i, c: (body(i), c)[1], 0, unroll=True)
                return None
            return lax.fori_loop(0, tiles, body, init, unroll=True)

        start[0:PROJECTED, :] = dense_ref[...]
        for t, (first, count, kind, index) in enumerate(tables):
            parts = []
            for k in range(count):
                slot = slot_ref[first + k]
                at = (slot % blocks_here) * (per * BLOCK_WIDTH)
                pieces = [
                    x_ref[slot // blocks_here, pl.ds(pl.multiple_of(at + h * BLOCK_WIDTH, 16), BLOCK_WIDTH), :]
                    for h in range(per)
                ]
                parts.append(jnp.concatenate(pieces, 1))
            block = parts[0] if count == 1 else jnp.concatenate(parts, 0)
            start[(t + 1) * PROJECTED : (t + 2) * PROJECTED, :] = dot(pts[kind][index], block).astype(BF)

        save(0).start()

        fetch(0).wait()
        hidden0 = dot(cit_ref[0], start[...]).astype(BF)
        small[0] = hidden0
        fetch(1).wait()

        def fwd0(i):
            s = start[tile(i), :].astype(F32)
            g = dot(cot_ref[0, tile(i), :], hidden0) + col_ref[tile(i), 0:1]
            gate0[tile(i), :] = g
            layer1[tile(i), :] = (s * g + s).astype(BF)

        loop(fwd0)
        save(1).start()
        fetch(2).wait()
        hidden1 = dot(cit_ref[1], layer1[...]).astype(BF)
        small[1] = hidden1
        fetch(3).wait()

        def fwd1(i, logit):
            s = start[tile(i), :].astype(F32)
            g = dot(cot_ref[1, tile(i), :], hidden1) + col_ref[tile(i), 1:2]
            gate1[tile(i), :] = g
            last = (s * g + layer1[tile(i), :].astype(F32)).astype(BF).astype(F32)
            term = last * col_ref[tile(i), 2:3]
            return logit + jnp.sum(term.reshape(tile_rows // 8, 8, rows), 0)

        partial = loop(fwd1, jnp.zeros((8, rows), F32))
        logit = jnp.sum(partial, 0, keepdims=True)
        depth = x_ref.shape[1]

        def gather_total(d, carry):
            return carry + x_ref[d][depth - 8 : depth, :].astype(F32)

        terms = lax.fori_loop(0, devices, gather_total, jnp.zeros((8, LANES), F32), unroll=8)
        total = jnp.sum(terms, 0, keepdims=True)[:, 0:1]
        scale = float(rows * devices) / total
        signal = scale * row_ref[0:1, :] * (jax.nn.sigmoid(logit) - row_ref[1:2, :])

        def bwd1(i):
            s = start[tile(i), :].astype(F32)
            low1[tile(i), :] = (s * (col_ref[tile(i), 2:3] * signal)).astype(BF)

        loop(bwd1)
        save(2).start()
        fetch(4).wait()
        hgrad1 = dot(co_ref[1], low1[...]).astype(BF)
        small[2] = hgrad1
        fetch(5).wait()

        def mid(i):
            s = start[tile(i), :].astype(F32)
            up2 = col_ref[tile(i), 2:3] * signal
            up1 = up2 + dot(ci_ref[1, tile(i), :], hgrad1)
            gate1[tile(i), :] = up1 + gate1[tile(i), :] * up2 + gate0[tile(i), :] * up1
            low0[tile(i), :] = (s * up1).astype(BF)

        loop(mid)
        save(3).start()
        fetch(6).wait()
        hgrad0 = dot(co_ref[0], low0[...]).astype(BF)
        small[3] = hgrad0
        fetch(7).wait()

        def fin(i):
            low[tile(i), :] = (gate1[tile(i), :] + dot(ci_ref[0, tile(i), :], hgrad0)).astype(BF)

        loop(fin)
        for t, (first, count, kind, index) in enumerate(tables):
            grad = low[(t + 1) * PROJECTED : (t + 2) * PROJECTED, :]
            block = dot(ps[kind][index], grad).astype(BF)
            for k in range(count):
                back_ref[slot_ref[first + k]] = block[k * BLOCK_WIDTH : (k + 1) * BLOCK_WIDTH, :]
        for n in range(len(written)):
            save(n).wait()

    return kernel


def make_grads(orders, splits, devices, chunk, chunk_pad):
    half = devices // 2
    colors = len(splits)

    def kernel(me_ref, start, layer1, low1, low0, small, *refs):
        los, his, acc = refs[:colors], refs[colors : 2 * colors], refs[2 * colors]
        group, rows = start.shape
        rank = small.shape[1]
        subs = group // chunk
        me = me_ref[0]
        acc[:, 0:rank] = dot(low1[...], small[1], NT)
        acc[:, rank : 2 * rank] = dot(layer1[...], small[2], NT)
        acc[:, 2 * rank : 3 * rank] = dot(low0[...], small[0], NT)
        acc[:, 3 * rank : 4 * rank] = dot(start[...], small[3], NT)
        ones = jnp.ones((8, rows), BF)
        biases = (dot(ones, low1[...], NT), dot(ones, low0[...], NT))
        spare = chunk_pad - chunk
        for s in range(subs):
            d = pl.program_id(0) * subs + s
            at = 0
            for which, cols in enumerate(splits):
                piece = acc[s * chunk : (s + 1) * chunk, at : at + cols]
                at += cols
                if which < 2:
                    tail = biases[which][0:spare, s * chunk : (s + 1) * chunk]
                    tail = jnp.concatenate([tail, jnp.zeros((spare, cols - chunk), F32)], 1)
                else:
                    tail = jnp.zeros((spare, cols), F32)
                value = jnp.concatenate([piece, tail], 0).astype(BF)
                place = position_of(d ^ me, orders[which])

                @pl.when(place < half)
                def _():
                    los[which][place] = value

                @pl.when(place >= half)
                def _():
                    his[which][place - half] = value

    return kernel


def add_pair(a, b):
    return (a.astype(F32) + b.astype(F32)).astype(BF)


def reduce_pieces(los, his, orders, devices):
    stages = len(orders[0])
    for k in range(stages):
        got = [
            lax.ppermute(h, AXES, [(i, i ^ o[k]) for i in range(devices)])
            for h, o in zip(his, orders)
        ]
        if k:
            got = lax.optimization_barrier(got)
        if k == stages - 1:
            return [add_pair(a, b)[0] for a, b in zip(los, got)]
        n = los[0].shape[0] // 2
        his = [add_pair(a[n:], b[n:]) for a, b in zip(los, got)]
        los = [add_pair(a[:n], b[:n]) for a, b in zip(los, got)]


def run(
    pooled,
    slot_of_block,
    dense_part,
    labels,
    sample_weight,
    proj_wide,
    proj_mid,
    proj_narrow,
    cross_in,
    cross_out,
    cross_bias,
    head_weight,
):
    dp_count, rep_count = lax.axis_size("dp"), lax.axis_size("rep")
    devices = dp_count * rep_count
    rows = labels.shape[0]
    blocks_here = pooled.shape[1]
    width = cross_bias.shape[1]
    rank = cross_in.shape[2]
    chunk = width // devices
    chunk_pad = (chunk // 8 + 1) * 8

    core, masks = exchange_basis(dp_count, rep_count)
    last = masks[-1:]
    others = masks[:-1]
    colors = 3
    orders = [
        core + [others[(c + i) % len(others)] for i in range(len(others))] + last for c in range(colors)
    ]
    splits = [(4 * rank // LANES + colors - 1 - c) // colors * LANES for c in range(colors)]
    tables = []
    first = 0
    for kind, proj in enumerate((proj_wide, proj_mid, proj_narrow)):
        per = proj.shape[1] // BLOCK_WIDTH
        for index in range(proj.shape[0]):
            tables.append((first, per, kind, index))
            first += per

    received = lax.all_to_all(pack(pooled, sample_weight, devices), AXES, 0, 0, tiled=True)
    row_data = jnp.stack([sample_weight, labels.astype(F32)])
    col_data = jnp.stack([cross_bias[0], cross_bias[1], head_weight], 1)
    me = lax.axis_index(AXES).astype(jnp.int32).reshape(1)

    smem = pl.BlockSpec(memory_space=pltpu.SMEM)
    vmem = pl.BlockSpec(memory_space=pltpu.VMEM)
    hbm = pl.BlockSpec(memory_space=pl.ANY)
    wide = jax.ShapeDtypeStruct((width, rows), BF)
    back, start, layer1, low1, low0, small = pl.pallas_call(
        make_step(tables, devices, blocks_here),
        in_specs=[smem] + [vmem] * 10 + [hbm] * 4,
        out_specs=[vmem] + [hbm] * 4 + [vmem],
        out_shape=[
            jax.ShapeDtypeStruct((blocks_here * devices, BLOCK_WIDTH, rows), BF),
            wide,
            wide,
            wide,
            wide,
            jax.ShapeDtypeStruct((4, rank, rows), BF),
        ],
        scratch_shapes=[pltpu.VMEM((width, rows), BF)] * 4
        + [
            pltpu.VMEM((2, rank, width), BF),
            pltpu.VMEM((2, width, rank), BF),
            pltpu.VMEM((2, width, rank), BF),
            pltpu.VMEM((2, rank, width), BF),
            pltpu.VMEM((width, rows), BF),
            pltpu.VMEM((width, rows), F32),
            pltpu.VMEM((width, rows), F32),
            pltpu.SemaphoreType.DMA((8,)),
            pltpu.SemaphoreType.DMA((4,)),
        ],
        compiler_params=pltpu.CompilerParams(vmem_limit_bytes=60 << 20),
        cost_estimate=pl.CostEstimate(flops=16 * width * rank * rows, bytes_accessed=20 << 20, transcendentals=rows),
        name="step",
    )(
        slot_of_block,
        received,
        dense_part,
        row_data,
        col_data,
        jnp.swapaxes(proj_wide, 1, 2),
        jnp.swapaxes(proj_mid, 1, 2),
        jnp.swapaxes(proj_narrow, 1, 2),
        proj_wide,
        proj_mid,
        proj_narrow,
        jnp.swapaxes(cross_in, 1, 2),
        cross_in,
        jnp.swapaxes(cross_out, 1, 2),
        cross_out,
    )
    back = back.reshape(devices, blocks_here * BLOCK_WIDTH, rows)
    back = lax.all_to_all(back, AXES, 0, 0, tiled=True)

    group = chunk
    while group % 16:
        group += chunk
    if width % (2 * group) == 0:
        group *= 2
    part = pl.BlockSpec((group, rows), lambda i: (i, 0))
    half = [jax.ShapeDtypeStruct((devices // 2, chunk_pad, c), BF) for c in splits]
    outs = pl.pallas_call(
        make_grads(orders, splits, devices, chunk, chunk_pad),
        grid=(width // group,),
        in_specs=[smem, part, part, part, part, pl.BlockSpec((4, rank, rows), lambda i: (0, 0, 0))],
        out_specs=[pl.BlockSpec(h.shape, lambda i: (0, 0, 0)) for h in half + half],
        out_shape=half + half,
        scratch_shapes=[pltpu.VMEM((group, 4 * rank), F32)],
        compiler_params=pltpu.CompilerParams(vmem_limit_bytes=60 << 20),
        cost_estimate=pl.CostEstimate(flops=8 * width * rank * rows, bytes_accessed=16 << 20, transcendentals=0),
        name="grads",
    )(me, start, layer1, low1, low0, small)
    los, his = list(outs[:colors]), list(outs[colors:])
    sums = reduce_pieces(los, his, orders, devices)
    pooled_grad = unpack(back)
    bias1, bias0 = sums[0][chunk, :chunk], sums[1][chunk, :chunk]
    flat = jnp.concatenate([x[:chunk] for x in sums], 1)
    out1, in1, out0, in0 = [flat[:, i * rank : (i + 1) * rank] for i in range(4)]
    grad_in = jnp.stack([in0, in1]).astype(F32)
    grad_out = jnp.stack([out0.T, out1.T]).astype(F32)
    grad_bias = jnp.stack([bias0, bias1]).astype(F32)
    return (pooled_grad, grad_in, grad_out, grad_bias)


def solution(mesh):
    return jax.shard_map(
        run,
        mesh=mesh,
        in_specs=(
            P(None, AXES, None),
            P(),
            P(None, AXES),
            P(AXES),
            P(AXES),
            P(),
            P(),
            P(),
            P(),
            P(),
            P(),
            P(),
        ),
        out_specs=(
            P(None, AXES, None),
            P(None, AXES, None),
            P(None, None, AXES),
            P(None, AXES),
        ),
        check_vma=False,
    )
```

```python
import jax
import jax.numpy as jnp
from jax import lax
from jax.experimental import pallas as pl
from jax.experimental.pallas import tpu as pltpu
from jax.sharding import PartitionSpec as P

BLOCK_WIDTH = 16
PROJECTED = 128
LANES = 128
AXES = ("dp", "rep")
NN = (((1,), (0,)), ((), ()))
NT = (((1,), (1,)), ((), ()))
BF = jnp.bfloat16
F32 = jnp.float32


def dot(a, b, dims=NN):
    return lax.dot_general(a, b, dims, preferred_element_type=F32)


def exchange_basis(dp_count, rep_count):
    bits = dp_count.bit_length() - 1
    low = bits - 2
    masks = []
    if low <= 2:
        masks += [1 << i for i in range(max(low, 0))]
    else:
        for base in range(0, low, 2):
            masks += [1 << base, 3 << base]
    if bits >= 2:
        masks += [1 << low, 2 << low]
    elif bits == 1:
        masks += [1]
    core = [1 << i for i in range(rep_count.bit_length() - 1)]
    return core, [m * rep_count for m in masks]


def basis_digits(index, masks):
    digits = {}
    for mask in sorted(masks, reverse=True):
        top = mask.bit_length() - 1
        bit = (index >> top) & 1
        digits[mask] = bit
        index = index ^ (bit * mask)
    return digits


def position_of(index, order):
    digits = basis_digits(index, order)
    place = 0
    for mask in order:
        place = place * 2 + digits[mask]
    return place


def pack_kernel(weight_ref, x_ref, out_ref, tmp_ref):
    group, depth, lanes = out_ref.shape
    width, blocks, span = x_ref.shape
    per = span // (group * lanes)
    for c in range(width):
        for m in range(group * per):
            tmp_ref[m, pl.ds(c, blocks, stride=width), :] = x_ref[c, :, m * lanes : (m + 1) * lanes].astype(F32)
    total = jnp.sum(jnp.sum(weight_ref[...], 0, keepdims=True), 1, keepdims=True)
    first = total.astype(BF).astype(F32)
    second = (total - first).astype(BF).astype(F32)
    third = total - first - second
    row = lax.broadcasted_iota(jnp.int32, (8, lanes), 0)
    tail = jnp.where(row == 0, first, jnp.where(row == 1, second, jnp.where(row == 2, third, 0.0)))
    for g in range(group):
        for j in range(blocks):
            for h in range(per):
                out_ref[g, (j * per + h) * width : (j * per + h + 1) * width, :] = tmp_ref[
                    g * per + h, j * width : (j + 1) * width, :
                ].astype(BF)
        out_ref[g, depth - 8 : depth, :] = tail.astype(BF)


def pack(pooled, weight, devices):
    width, blocks, batch = pooled.shape
    rows = batch // devices
    per = rows // LANES
    group = 16
    depth = blocks * per * width + 8
    return pl.pallas_call(
        pack_kernel,
        grid=(devices // group,),
        in_specs=[
            pl.BlockSpec((per, LANES), lambda i: (0, 0)),
            pl.BlockSpec((width, blocks, group * rows), lambda i: (0, 0, i)),
        ],
        out_specs=pl.BlockSpec((group, depth, LANES), lambda i: (i, 0, 0)),
        out_shape=jax.ShapeDtypeStruct((devices, depth, LANES), BF),
        scratch_shapes=[pltpu.VMEM((group * per, blocks * width, LANES), F32)],
        name="pack",
    )(weight.reshape(per, LANES), pooled)


def unpack_kernel(x_ref, out_ref, tmp_ref):
    group, _, rows = x_ref.shape
    width, blocks, _ = out_ref.shape
    lanes = tmp_ref.shape[2]
    per = rows // lanes
    for m in range(group * per):
        at = (m % per) * lanes
        tmp_ref[m] = x_ref[m // per, :, at : at + lanes].astype(F32)
        for c in range(width):
            out_ref[c, :, m * lanes : (m + 1) * lanes] = tmp_ref[m, pl.ds(c, blocks, stride=width), :]


def unpack(received):
    width = BLOCK_WIDTH
    devices, both, rows = received.shape
    blocks = both // width
    group = 8
    return pl.pallas_call(
        unpack_kernel,
        grid=(devices // group,),
        in_specs=[pl.BlockSpec((group, both, rows), lambda i: (i, 0, 0))],
        out_specs=pl.BlockSpec((width, blocks, group * rows), lambda i: (0, 0, i)),
        out_shape=jax.ShapeDtypeStruct((width, blocks, devices * rows), F32),
        scratch_shapes=[pltpu.VMEM((group * rows // LANES, both, LANES), F32)],
        name="unpack",
    )(received)


def make_step(tables, devices, blocks_here):
    def kernel(
        slot_ref,
        x_ref,
        dense_ref,
        row_ref,
        col_hbm,
        pt0,
        pt1,
        pt2,
        p0,
        p1,
        p2,
        cit_hbm,
        ci_hbm,
        cot_hbm,
        co_hbm,
        back_ref,
        start_hbm,
        layer1_hbm,
        low1_hbm,
        low0_hbm,
        small,
        start,
        layer1,
        low1,
        low0,
        cit_ref,
        ci_ref,
        cot_ref,
        co_ref,
        low,
        gate0,
        gate1,
        col_ref,
        sems,
        out_sems,
    ):
        pts, ps = (pt0, pt1, pt2), (p0, p1, p2)
        width, rows = start.shape
        tile_rows = 3 * PROJECTED
        tiles = width // tile_rows
        per = rows // LANES

        names = {"cit": (cit_hbm, cit_ref), "cot": (cot_hbm, cot_ref), "co": (co_hbm, co_ref), "ci": (ci_hbm, ci_ref)}
        uses = [("cit", 0), ("cot", 0), ("cit", 1), ("cot", 1), ("co", 1), ("ci", 1), ("co", 0), ("ci", 0)]

        def fetch(n):
            if n == len(uses):
                return pltpu.make_async_copy(col_hbm, col_ref, sems.at[n])
            name, layer = uses[n]
            source, target = names[name]
            return pltpu.make_async_copy(source.at[layer], target.at[layer], sems.at[n])

        for n in (0, len(uses), *range(1, len(uses))):
            fetch(n).start()
        written = ((start, start_hbm), (layer1, layer1_hbm), (low1, low1_hbm), (low0, low0_hbm))

        def save(n):
            source, target = written[n]
            return pltpu.make_async_copy(source, target, out_sems.at[n])

        def tile(i):
            return pl.ds(pl.multiple_of(i * tile_rows, tile_rows), tile_rows)

        def loop(body, init=None):
            if init is None:
                lax.fori_loop(0, tiles, lambda i, c: (body(i), c)[1], 0, unroll=True)
                return None
            return lax.fori_loop(0, tiles, body, init, unroll=True)

        start[0:PROJECTED, :] = dense_ref[...]
        for t, (first, count, kind, index) in enumerate(tables):
            parts = []
            for k in range(count):
                slot = slot_ref[first + k]
                at = (slot % blocks_here) * (per * BLOCK_WIDTH)
                pieces = [
                    x_ref[slot // blocks_here, pl.ds(pl.multiple_of(at + h * BLOCK_WIDTH, 16), BLOCK_WIDTH), :]
                    for h in range(per)
                ]
                parts.append(jnp.concatenate(pieces, 1))
            block = parts[0] if count == 1 else jnp.concatenate(parts, 0)
            start[(t + 1) * PROJECTED : (t + 2) * PROJECTED, :] = dot(pts[kind][index], block).astype(BF)

        save(0).start()

        fetch(0).wait()
        hidden0 = dot(cit_ref[0], start[...]).astype(BF)
        small[0] = hidden0
        fetch(len(uses)).wait()
        fetch(1).wait()

        def fwd0(i):
            s = start[tile(i), :].astype(F32)
            g = dot(cot_ref[0, tile(i), :], hidden0) + col_ref[tile(i), 0:1]
            gate0[tile(i), :] = g
            layer1[tile(i), :] = (s * g + s).astype(BF)

        loop(fwd0)
        save(1).start()
        fetch(2).wait()
        hidden1 = dot(cit_ref[1], layer1[...]).astype(BF)
        small[1] = hidden1
        fetch(3).wait()

        def fwd1(i, logit):
            s = start[tile(i), :].astype(F32)
            g = dot(cot_ref[1, tile(i), :], hidden1) + col_ref[tile(i), 1:2]
            gate1[tile(i), :] = g
            last = (s * g + layer1[tile(i), :].astype(F32)).astype(BF).astype(F32)
            term = last * col_ref[tile(i), 2:3]
            return logit + jnp.sum(term.reshape(tile_rows // 8, 8, rows), 0)

        partial = loop(fwd1, jnp.zeros((8, rows), F32))
        logit = jnp.sum(partial, 0, keepdims=True)
        depth = x_ref.shape[1]

        def gather_total(d, carry):
            return carry + x_ref[d][depth - 8 : depth, :].astype(F32)

        terms = lax.fori_loop(0, devices, gather_total, jnp.zeros((8, LANES), F32), unroll=8)
        total = jnp.sum(terms, 0, keepdims=True)[:, 0:1]
        scale = float(rows * devices) / total
        signal = scale * row_ref[0:1, :] * (jax.nn.sigmoid(logit) - row_ref[1:2, :])

        def bwd1(i):
            s = start[tile(i), :].astype(F32)
            low1[tile(i), :] = (s * (col_ref[tile(i), 2:3] * signal)).astype(BF)

        loop(bwd1)
        save(2).start()
        fetch(4).wait()
        hgrad1 = dot(co_ref[1], low1[...]).astype(BF)
        small[2] = hgrad1
        fetch(5).wait()

        def mid(i):
            s = start[tile(i), :].astype(F32)
            up2 = col_ref[tile(i), 2:3] * signal
            up1 = up2 + dot(ci_ref[1, tile(i), :], hgrad1)
            gate1[tile(i), :] = up1 + gate1[tile(i), :] * up2 + gate0[tile(i), :] * up1
            low0[tile(i), :] = (s * up1).astype(BF)

        loop(mid)
        save(3).start()
        fetch(6).wait()
        hgrad0 = dot(co_ref[0], low0[...]).astype(BF)
        small[3] = hgrad0
        fetch(7).wait()

        def fin(i):
            low[tile(i), :] = (gate1[tile(i), :] + dot(ci_ref[0, tile(i), :], hgrad0)).astype(BF)

        loop(fin)
        for t, (first, count, kind, index) in enumerate(tables):
            grad = low[(t + 1) * PROJECTED : (t + 2) * PROJECTED, :]
            block = dot(ps[kind][index], grad).astype(BF)
            for k in range(count):
                back_ref[slot_ref[first + k]] = block[k * BLOCK_WIDTH : (k + 1) * BLOCK_WIDTH, :]
        for n in range(len(written)):
            save(n).wait()

    return kernel


def make_grads(pieces, biases, orders, cols, devices, chunk, chunk_pad):
    half = devices // 2
    colors = len(pieces)

    def kernel(me_ref, small, *refs):
        wides, (los, his, acc) = refs[: -2 * colors - 1], (
            refs[-2 * colors - 1 : -colors - 1],
            refs[-colors - 1 : -1],
            refs[-1],
        )
        group, rows = wides[0].shape
        subs = group // chunk
        me = me_ref[0]
        spare = chunk_pad - chunk
        at = 0
        for parts in pieces:
            for wide, low, first, last in parts:
                acc[:, at : at + last - first] = dot(wides[wide][...], small[low, first:last, :], NT)
                at += last - first
        ones = jnp.ones((8, rows), BF)
        sums = [None if w is None else dot(ones, wides[w][...], NT) for w in biases]
        for s in range(subs):
            d = pl.program_id(0) * subs + s
            at = 0
            for which in range(colors):
                piece = acc[s * chunk : (s + 1) * chunk, at : at + cols[which]]
                at += cols[which]
                if sums[which] is not None:
                    tail = sums[which][0:spare, s * chunk : (s + 1) * chunk]
                    tail = jnp.concatenate([tail, jnp.zeros((spare, cols[which] - chunk), F32)], 1)
                else:
                    tail = jnp.zeros((spare, cols[which]), F32)
                value = jnp.concatenate([piece, tail], 0).astype(BF)
                place = position_of(d ^ me, orders[which])

                @pl.when(place < half)
                def _():
                    los[which][place] = value

                @pl.when(place >= half)
                def _():
                    his[which][place - half] = value

    return kernel


def weight_grads(me, small, wides, pieces, biases, orders, devices, chunk, chunk_pad):
    width, rows = wides[0].shape
    group = chunk
    while group % 16:
        group += chunk
    if width % (2 * group) == 0:
        group *= 2
    colors = len(pieces)
    cols = [sum(last - first for _, _, first, last in p) for p in pieces]
    part = pl.BlockSpec((group, rows), lambda i: (i, 0))
    half = [jax.ShapeDtypeStruct((devices // 2, chunk_pad, c), BF) for c in cols]
    outs = pl.pallas_call(
        make_grads(pieces, biases, orders, cols, devices, chunk, chunk_pad),
        grid=(width // group,),
        in_specs=[pl.BlockSpec(memory_space=pltpu.SMEM), pl.BlockSpec(small.shape, lambda i: (0, 0, 0))]
        + [part] * len(wides),
        out_specs=[pl.BlockSpec(h.shape, lambda i: (0, 0, 0)) for h in half + half],
        out_shape=half + half,
        scratch_shapes=[pltpu.VMEM((group, sum(cols)), F32)],
        compiler_params=pltpu.CompilerParams(vmem_limit_bytes=46 << 20),
        cost_estimate=pl.CostEstimate(
            flops=2 * width * sum(cols) * rows, bytes_accessed=4 * width * sum(cols), transcendentals=0
        ),
    )(me, small, *wides)
    return list(outs[:colors]), list(outs[colors:])


def add_pair(a, b):
    return (a.astype(F32) + b.astype(F32)).astype(BF)


def reduce_pieces(los, his, orders, devices):
    stages = len(orders[0])
    for k in range(stages):
        got = [
            lax.ppermute(h, AXES, [(i, i ^ o[k]) for i in range(devices)])
            for h, o in zip(his, orders)
        ]
        if k:
            got = lax.optimization_barrier(got)
        if k == stages - 1:
            return [add_pair(a, b)[0] for a, b in zip(los, got)]
        n = los[0].shape[0] // 2
        his = [add_pair(a[n:], b[n:]) for a, b in zip(los, got)]
        los = [add_pair(a[:n], b[:n]) for a, b in zip(los, got)]


def run(
    pooled,
    slot_of_block,
    dense_part,
    labels,
    sample_weight,
    proj_wide,
    proj_mid,
    proj_narrow,
    cross_in,
    cross_out,
    cross_bias,
    head_weight,
):
    dp_count, rep_count = lax.axis_size("dp"), lax.axis_size("rep")
    devices = dp_count * rep_count
    rows = labels.shape[0]
    blocks_here = pooled.shape[1]
    width = cross_bias.shape[1]
    rank = cross_in.shape[2]
    chunk = width // devices
    chunk_pad = (chunk // 8 + 1) * 8

    core, masks = exchange_basis(dp_count, rep_count)
    last = masks[-1:]
    others = masks[:-1]
    colors = 3
    orders = [
        core + [others[(c + i) % len(others)] for i in range(len(others))] + last for c in range(colors)
    ]
    splits = [(4 * rank // LANES + colors - 1 - c) // colors * LANES for c in range(colors)]
    tables = []
    first = 0
    for kind, proj in enumerate((proj_wide, proj_mid, proj_narrow)):
        per = proj.shape[1] // BLOCK_WIDTH
        for index in range(proj.shape[0]):
            tables.append((first, per, kind, index))
            first += per

    received = lax.all_to_all(pack(pooled, sample_weight, devices), AXES, 0, 0, tiled=True)
    row_data = jnp.stack([sample_weight, labels.astype(F32)])
    col_data = jnp.stack([cross_bias[0], cross_bias[1], head_weight], 1)
    me = lax.axis_index(AXES).astype(jnp.int32).reshape(1)

    smem = pl.BlockSpec(memory_space=pltpu.SMEM)
    vmem = pl.BlockSpec(memory_space=pltpu.VMEM)
    hbm = pl.BlockSpec(memory_space=pl.ANY)
    wide = jax.ShapeDtypeStruct((width, rows), BF)
    back, start, layer1, low1, low0, small = pl.pallas_call(
        make_step(tables, devices, blocks_here),
        in_specs=[smem] + [vmem] * 3 + [hbm] + [vmem] * 6 + [hbm] * 4,
        out_specs=[vmem] + [hbm] * 4 + [vmem],
        out_shape=[
            jax.ShapeDtypeStruct((blocks_here * devices, BLOCK_WIDTH, rows), BF),
            wide,
            wide,
            wide,
            wide,
            jax.ShapeDtypeStruct((4, rank, rows), BF),
        ],
        scratch_shapes=[pltpu.VMEM((width, rows), BF)] * 4
        + [
            pltpu.VMEM((2, rank, width), BF),
            pltpu.VMEM((2, width, rank), BF),
            pltpu.VMEM((2, width, rank), BF),
            pltpu.VMEM((2, rank, width), BF),
            pltpu.VMEM((width, rows), BF),
            pltpu.VMEM((width, rows), F32),
            pltpu.VMEM((width, rows), F32),
            pltpu.VMEM((width, 3), F32),
            pltpu.SemaphoreType.DMA((9,)),
            pltpu.SemaphoreType.DMA((4,)),
        ],
        compiler_params=pltpu.CompilerParams(vmem_limit_bytes=60 << 20),
        cost_estimate=pl.CostEstimate(flops=16 * width * rank * rows, bytes_accessed=20 << 20, transcendentals=rows),
        name="step",
    )(
        slot_of_block,
        received,
        dense_part,
        row_data,
        col_data,
        jnp.swapaxes(proj_wide, 1, 2),
        jnp.swapaxes(proj_mid, 1, 2),
        jnp.swapaxes(proj_narrow, 1, 2),
        proj_wide,
        proj_mid,
        proj_narrow,
        jnp.swapaxes(cross_in, 1, 2),
        cross_in,
        jnp.swapaxes(cross_out, 1, 2),
        cross_out,
    )
    back = back.reshape(devices, blocks_here * BLOCK_WIDTH, rows)
    back = lax.all_to_all(back, AXES, 0, 0, tiled=True)

    cut = splits[0] - rank
    fixed = (devices, chunk, chunk_pad)
    los, his = weight_grads(
        me, small, (low1, layer1, low0, start),
        [[(0, 1, 0, rank), (1, 2, 0, cut)], [(1, 2, cut, rank), (2, 0, 0, rank)], [(3, 3, 0, rank)]],
        [0, 2, None], orders, *fixed,
    )
    sums = reduce_pieces(los, his, orders, devices)
    pooled_grad = unpack(back)
    bias1, bias0 = sums[0][chunk, :chunk], sums[1][chunk, :chunk]
    flat = jnp.concatenate([x[:chunk] for x in sums], 1).astype(F32)
    out1, in1, out0, in0 = [flat[:, i * rank : (i + 1) * rank] for i in range(4)]
    grad_in = jnp.transpose(jnp.stack([in0, in1], 1), (1, 0, 2))
    grad_out = jnp.transpose(jnp.stack([out0, out1], 1), (1, 2, 0))
    grad_bias = jnp.stack([bias0, bias1]).astype(F32)
    return (pooled_grad, grad_in, grad_out, grad_bias)


def solution(mesh):
    return jax.shard_map(
        run,
        mesh=mesh,
        in_specs=(
            P(None, AXES, None),
            P(),
            P(None, AXES),
            P(AXES),
            P(AXES),
            P(),
            P(),
            P(),
            P(),
            P(),
            P(),
            P(),
        ),
        out_specs=(
            P(None, AXES, None),
            P(None, AXES, None),
            P(None, None, AXES),
            P(None, AXES),
        ),
        check_vma=False,
    )
```

```python
import jax
import jax.numpy as jnp
from jax import lax
from jax.experimental import pallas as pl
from jax.experimental.pallas import tpu as pltpu
from jax.sharding import PartitionSpec as P

BLOCK_WIDTH = 16
PROJECTED = 128
LANES = 128
AXES = ("dp", "rep")
NN = (((1,), (0,)), ((), ()))
NT = (((1,), (1,)), ((), ()))
BF = jnp.bfloat16
F32 = jnp.float32


def dot(a, b, dims=NN):
    return lax.dot_general(a, b, dims, preferred_element_type=F32)


def exchange_basis(dp_count, rep_count):
    bits = dp_count.bit_length() - 1
    low = bits - 2
    masks = []
    if low <= 2:
        masks += [1 << i for i in range(max(low, 0))]
    else:
        for base in range(0, low, 2):
            masks += [1 << base, 3 << base]
    if bits >= 2:
        masks += [1 << low, 2 << low]
    elif bits == 1:
        masks += [1]
    core = [1 << i for i in range(rep_count.bit_length() - 1)]
    return core, [m * rep_count for m in masks]


def basis_digits(index, masks):
    digits = {}
    for mask in sorted(masks, reverse=True):
        top = mask.bit_length() - 1
        bit = (index >> top) & 1
        digits[mask] = bit
        index = index ^ (bit * mask)
    return digits


def position_of(index, order):
    digits = basis_digits(index, order)
    place = 0
    for mask in order:
        place = place * 2 + digits[mask]
    return place


def pack_kernel(weight_ref, x_ref, out_ref, tmp_ref):
    group, depth, lanes = out_ref.shape
    width, blocks, span = x_ref.shape
    per = span // (group * lanes)
    for c in range(width):
        for m in range(group * per):
            tmp_ref[m, pl.ds(c, blocks, stride=width), :] = x_ref[c, :, m * lanes : (m + 1) * lanes].astype(F32)
    total = jnp.sum(jnp.sum(weight_ref[...], 0, keepdims=True), 1, keepdims=True)
    first = total.astype(BF).astype(F32)
    second = (total - first).astype(BF).astype(F32)
    third = total - first - second
    row = lax.broadcasted_iota(jnp.int32, (8, lanes), 0)
    tail = jnp.where(row == 0, first, jnp.where(row == 1, second, jnp.where(row == 2, third, 0.0)))
    for g in range(group):
        for j in range(blocks):
            for h in range(per):
                out_ref[g, (j * per + h) * width : (j * per + h + 1) * width, :] = tmp_ref[
                    g * per + h, j * width : (j + 1) * width, :
                ].astype(BF)
        out_ref[g, depth - 8 : depth, :] = tail.astype(BF)


def pack(pooled, weight, devices):
    width, blocks, batch = pooled.shape
    rows = batch // devices
    per = rows // LANES
    group = 16
    depth = blocks * per * width + 8
    return pl.pallas_call(
        pack_kernel,
        grid=(devices // group,),
        in_specs=[
            pl.BlockSpec((per, LANES), lambda i: (0, 0)),
            pl.BlockSpec((width, blocks, group * rows), lambda i: (0, 0, i)),
        ],
        out_specs=pl.BlockSpec((group, depth, LANES), lambda i: (i, 0, 0)),
        out_shape=jax.ShapeDtypeStruct((devices, depth, LANES), BF),
        scratch_shapes=[pltpu.VMEM((group * per, blocks * width, LANES), F32)],
        name="pack",
    )(weight.reshape(per, LANES), pooled)


def unpack_kernel(x_ref, out_ref, tmp_ref):
    group, _, rows = x_ref.shape
    width, blocks, _ = out_ref.shape
    lanes = tmp_ref.shape[2]
    per = rows // lanes
    for m in range(group * per):
        at = (m % per) * lanes
        tmp_ref[m] = x_ref[m // per, :, at : at + lanes].astype(F32)
        for c in range(width):
            out_ref[c, :, m * lanes : (m + 1) * lanes] = tmp_ref[m, pl.ds(c, blocks, stride=width), :]


def unpack(received):
    width = BLOCK_WIDTH
    devices, both, rows = received.shape
    blocks = both // width
    group = 8
    return pl.pallas_call(
        unpack_kernel,
        grid=(devices // group,),
        in_specs=[pl.BlockSpec((group, both, rows), lambda i: (i, 0, 0))],
        out_specs=pl.BlockSpec((width, blocks, group * rows), lambda i: (0, 0, i)),
        out_shape=jax.ShapeDtypeStruct((width, blocks, devices * rows), F32),
        scratch_shapes=[pltpu.VMEM((group * rows // LANES, both, LANES), F32)],
        name="unpack",
    )(received)


def make_step(tables, devices, blocks_here):
    def kernel(
        slot_ref,
        x_ref,
        dense_ref,
        row_ref,
        col_hbm,
        pt0,
        pt1,
        pt2,
        p0,
        p1,
        p2,
        cit_hbm,
        ci_hbm,
        cot_hbm,
        co_hbm,
        back_ref,
        start_hbm,
        layer1_hbm,
        low1_hbm,
        low0_hbm,
        small,
        start,
        layer1,
        low1,
        low0,
        cit_ref,
        ci_ref,
        cot_ref,
        co_ref,
        low,
        gate0,
        gate1,
        col_ref,
        sems,
        out_sems,
    ):
        pts, ps = (pt0, pt1, pt2), (p0, p1, p2)
        width, rows = start.shape
        tile_rows = 3 * PROJECTED
        tiles = width // tile_rows
        per = rows // LANES

        names = {"cit": (cit_hbm, cit_ref), "cot": (cot_hbm, cot_ref), "co": (co_hbm, co_ref), "ci": (ci_hbm, ci_ref)}
        uses = [("cit", 0), ("cot", 0), ("cit", 1), ("cot", 1), ("co", 1), ("ci", 1), ("co", 0), ("ci", 0)]

        def fetch(n):
            if n == len(uses):
                return pltpu.make_async_copy(col_hbm, col_ref, sems.at[n])
            name, layer = uses[n]
            source, target = names[name]
            return pltpu.make_async_copy(source.at[layer], target.at[layer], sems.at[n])

        for n in (0, len(uses), *range(1, len(uses))):
            fetch(n).start()
        written = ((start, start_hbm), (layer1, layer1_hbm), (low1, low1_hbm), (low0, low0_hbm))

        def save(n):
            source, target = written[n]
            return pltpu.make_async_copy(source, target, out_sems.at[n])

        def tile(i):
            return pl.ds(pl.multiple_of(i * tile_rows, tile_rows), tile_rows)

        def loop(body, init=None):
            if init is None:
                lax.fori_loop(0, tiles, lambda i, c: (body(i), c)[1], 0, unroll=True)
                return None
            return lax.fori_loop(0, tiles, body, init, unroll=True)

        start[0:PROJECTED, :] = dense_ref[...]
        for t, (first, count, kind, index) in enumerate(tables):
            parts = []
            for k in range(count):
                slot = slot_ref[first + k]
                at = (slot % blocks_here) * (per * BLOCK_WIDTH)
                pieces = [
                    x_ref[slot // blocks_here, pl.ds(pl.multiple_of(at + h * BLOCK_WIDTH, 16), BLOCK_WIDTH), :]
                    for h in range(per)
                ]
                parts.append(jnp.concatenate(pieces, 1))
            block = parts[0] if count == 1 else jnp.concatenate(parts, 0)
            start[(t + 1) * PROJECTED : (t + 2) * PROJECTED, :] = dot(pts[kind][index], block).astype(BF)

        save(0).start()

        fetch(0).wait()
        hidden0 = dot(cit_ref[0], start[...]).astype(BF)
        small[0] = hidden0
        fetch(len(uses)).wait()
        fetch(1).wait()

        def fwd0(i):
            s = start[tile(i), :].astype(F32)
            g = dot(cot_ref[0, tile(i), :], hidden0) + col_ref[tile(i), 0:1]
            gate0[tile(i), :] = g
            layer1[tile(i), :] = (s * g + s).astype(BF)

        loop(fwd0)
        save(1).start()
        fetch(2).wait()
        hidden1 = dot(cit_ref[1], layer1[...]).astype(BF)
        small[1] = hidden1
        fetch(3).wait()

        def fwd1(i, logit):
            s = start[tile(i), :].astype(F32)
            g = dot(cot_ref[1, tile(i), :], hidden1) + col_ref[tile(i), 1:2]
            gate1[tile(i), :] = g
            last = (s * g + layer1[tile(i), :].astype(F32)).astype(BF).astype(F32)
            term = last * col_ref[tile(i), 2:3]
            return logit + jnp.sum(term.reshape(tile_rows // 8, 8, rows), 0)

        partial = loop(fwd1, jnp.zeros((8, rows), F32))
        logit = jnp.sum(partial, 0, keepdims=True)
        depth = x_ref.shape[1]

        def gather_total(d, carry):
            return carry + x_ref[d][depth - 8 : depth, :].astype(F32)

        terms = lax.fori_loop(0, devices, gather_total, jnp.zeros((8, LANES), F32), unroll=8)
        total = jnp.sum(terms, 0, keepdims=True)[:, 0:1]
        scale = float(rows * devices) / total
        signal = scale * row_ref[0:1, :] * (jax.nn.sigmoid(logit) - row_ref[1:2, :])

        def bwd1(i):
            s = start[tile(i), :].astype(F32)
            low1[tile(i), :] = (s * (col_ref[tile(i), 2:3] * signal)).astype(BF)

        loop(bwd1)
        save(2).start()
        fetch(4).wait()
        hgrad1 = dot(co_ref[1], low1[...]).astype(BF)
        small[2] = hgrad1
        fetch(5).wait()

        def mid(i):
            s = start[tile(i), :].astype(F32)
            up2 = col_ref[tile(i), 2:3] * signal
            up1 = up2 + dot(ci_ref[1, tile(i), :], hgrad1)
            gate1[tile(i), :] = up1 + gate1[tile(i), :] * up2 + gate0[tile(i), :] * up1
            low0[tile(i), :] = (s * up1).astype(BF)

        loop(mid)
        save(3).start()
        fetch(6).wait()
        hgrad0 = dot(co_ref[0], low0[...]).astype(BF)
        small[3] = hgrad0
        fetch(7).wait()

        def fin(i):
            low[tile(i), :] = (gate1[tile(i), :] + dot(ci_ref[0, tile(i), :], hgrad0)).astype(BF)

        loop(fin)
        for t, (first, count, kind, index) in enumerate(tables):
            grad = low[(t + 1) * PROJECTED : (t + 2) * PROJECTED, :]
            block = dot(ps[kind][index], grad).astype(BF)
            for k in range(count):
                back_ref[slot_ref[first + k]] = block[k * BLOCK_WIDTH : (k + 1) * BLOCK_WIDTH, :]
        for n in range(len(written)):
            save(n).wait()

    return kernel


def make_grads(pieces, biases, orders, cols, devices, chunk, chunk_pad):
    half = devices // 2
    colors = len(pieces)

    def kernel(me_ref, small, *refs):
        wides, (los, his, acc) = refs[: -2 * colors - 1], (
            refs[-2 * colors - 1 : -colors - 1],
            refs[-colors - 1 : -1],
            refs[-1],
        )
        group, rows = wides[0].shape
        subs = group // chunk
        me = me_ref[0]
        spare = chunk_pad - chunk
        at = 0
        for parts in pieces:
            for wide, low, first, last in parts:
                acc[:, at : at + last - first] = dot(wides[wide][...], small[low, first:last, :], NT)
                at += last - first
        ones = jnp.ones((8, rows), BF)
        sums = [None if w is None else dot(ones, wides[w][...], NT) for w in biases]
        for s in range(subs):
            d = pl.program_id(0) * subs + s
            at = 0
            for which in range(colors):
                piece = acc[s * chunk : (s + 1) * chunk, at : at + cols[which]]
                at += cols[which]
                if sums[which] is not None:
                    tail = sums[which][0:spare, s * chunk : (s + 1) * chunk]
                    tail = jnp.concatenate([tail, jnp.zeros((spare, cols[which] - chunk), F32)], 1)
                else:
                    tail = jnp.zeros((spare, cols[which]), F32)
                value = jnp.concatenate([piece, tail], 0).astype(BF)
                place = position_of(d ^ me, orders[which])

                @pl.when(place < half)
                def _():
                    los[which][place] = value

                @pl.when(place >= half)
                def _():
                    his[which][place - half] = value

    return kernel


def weight_grads(me, small, wides, pieces, biases, orders, devices, chunk, chunk_pad):
    width, rows = wides[0].shape
    group = chunk
    while group % 16:
        group += chunk
    if width % (2 * group) == 0:
        group *= 2
    colors = len(pieces)
    cols = [sum(last - first for _, _, first, last in p) for p in pieces]
    part = pl.BlockSpec((group, rows), lambda i: (i, 0))
    half = [jax.ShapeDtypeStruct((devices // 2, chunk_pad, c), BF) for c in cols]
    outs = pl.pallas_call(
        make_grads(pieces, biases, orders, cols, devices, chunk, chunk_pad),
        grid=(width // group,),
        in_specs=[pl.BlockSpec(memory_space=pltpu.SMEM), pl.BlockSpec(small.shape, lambda i: (0, 0, 0))]
        + [part] * len(wides),
        out_specs=[pl.BlockSpec(h.shape, lambda i: (0, 0, 0)) for h in half + half],
        out_shape=half + half,
        scratch_shapes=[pltpu.VMEM((group, sum(cols)), F32)],
        compiler_params=pltpu.CompilerParams(vmem_limit_bytes=46 << 20),
        cost_estimate=pl.CostEstimate(
            flops=2 * width * sum(cols) * rows, bytes_accessed=4 * width * sum(cols), transcendentals=0
        ),
    )(me, small, *wides)
    return list(outs[:colors]), list(outs[colors:])


def add_pair(a, b):
    return (a.astype(F32) + b.astype(F32)).astype(BF)


def reduce_pieces(los, his, orders, devices):
    stages = len(orders[0])
    for k in range(stages):
        got = [
            lax.ppermute(h, AXES, [(i, i ^ o[k]) for i in range(devices)])
            for h, o in zip(his, orders)
        ]
        if k:
            got = lax.optimization_barrier(got)
        if k == stages - 1:
            return los, list(got)
        n = los[0].shape[0] // 2
        his = [add_pair(a[n:], b[n:]) for a, b in zip(los, got)]
        los = [add_pair(a[:n], b[:n]) for a, b in zip(los, got)]


def finish(mine, got, rank, chunk):
    colors = len(mine)

    def kernel(*refs):
        in_ref, out_ref, bias_ref = refs[2 * colors :]
        sums = [a[0].astype(F32) + b[0].astype(F32) for a, b in zip(refs[:colors], refs[colors : 2 * colors])]
        targets = ((out_ref, 1), (in_ref, 1), (out_ref, 0), (in_ref, 0))
        at = 0
        for x in sums:
            done = 0
            while done < x.shape[1]:
                target, layer = targets[at // rank]
                size = min(x.shape[1] - done, rank - at % rank)
                target[:, layer, at % rank : at % rank + size] = x[:chunk, done : done + size]
                done += size
                at += size
        bias_ref[0:1, :] = sums[1][chunk : chunk + 1, :chunk]
        bias_ref[1:2, :] = sums[0][chunk : chunk + 1, :chunk]

    vmem = pl.BlockSpec(memory_space=pltpu.VMEM)
    wide = jax.ShapeDtypeStruct((chunk, 2, rank), F32)
    return pl.pallas_call(
        kernel,
        in_specs=[vmem] * (2 * colors),
        out_specs=[vmem] * 3,
        out_shape=[wide, wide, jax.ShapeDtypeStruct((2, chunk), F32)],
        compiler_params=pltpu.CompilerParams(vmem_limit_bytes=16 << 20),
        name="finish",
    )(*mine, *got)


def run(
    pooled,
    slot_of_block,
    dense_part,
    labels,
    sample_weight,
    proj_wide,
    proj_mid,
    proj_narrow,
    cross_in,
    cross_out,
    cross_bias,
    head_weight,
):
    dp_count, rep_count = lax.axis_size("dp"), lax.axis_size("rep")
    devices = dp_count * rep_count
    rows = labels.shape[0]
    blocks_here = pooled.shape[1]
    width = cross_bias.shape[1]
    rank = cross_in.shape[2]
    chunk = width // devices
    chunk_pad = (chunk // 8 + 1) * 8

    core, masks = exchange_basis(dp_count, rep_count)
    last = masks[-1:]
    others = masks[:-1]
    colors = 3
    orders = [
        core + [others[(c + i) % len(others)] for i in range(len(others))] + last for c in range(colors)
    ]
    splits = [(4 * rank // LANES + colors - 1 - c) // colors * LANES for c in range(colors)]
    tables = []
    first = 0
    for kind, proj in enumerate((proj_wide, proj_mid, proj_narrow)):
        per = proj.shape[1] // BLOCK_WIDTH
        for index in range(proj.shape[0]):
            tables.append((first, per, kind, index))
            first += per

    received = lax.all_to_all(pack(pooled, sample_weight, devices), AXES, 0, 0, tiled=True)
    row_data = jnp.stack([sample_weight, labels.astype(F32)])
    col_data = jnp.stack([cross_bias[0], cross_bias[1], head_weight], 1)
    me = lax.axis_index(AXES).astype(jnp.int32).reshape(1)

    smem = pl.BlockSpec(memory_space=pltpu.SMEM)
    vmem = pl.BlockSpec(memory_space=pltpu.VMEM)
    hbm = pl.BlockSpec(memory_space=pl.ANY)
    wide = jax.ShapeDtypeStruct((width, rows), BF)
    back, start, layer1, low1, low0, small = pl.pallas_call(
        make_step(tables, devices, blocks_here),
        in_specs=[smem] + [vmem] * 3 + [hbm] + [vmem] * 6 + [hbm] * 4,
        out_specs=[vmem] + [hbm] * 4 + [vmem],
        out_shape=[
            jax.ShapeDtypeStruct((blocks_here * devices, BLOCK_WIDTH, rows), BF),
            wide,
            wide,
            wide,
            wide,
            jax.ShapeDtypeStruct((4, rank, rows), BF),
        ],
        scratch_shapes=[pltpu.VMEM((width, rows), BF)] * 4
        + [
            pltpu.VMEM((2, rank, width), BF),
            pltpu.VMEM((2, width, rank), BF),
            pltpu.VMEM((2, width, rank), BF),
            pltpu.VMEM((2, rank, width), BF),
            pltpu.VMEM((width, rows), BF),
            pltpu.VMEM((width, rows), F32),
            pltpu.VMEM((width, rows), F32),
            pltpu.VMEM((width, 3), F32),
            pltpu.SemaphoreType.DMA((9,)),
            pltpu.SemaphoreType.DMA((4,)),
        ],
        compiler_params=pltpu.CompilerParams(vmem_limit_bytes=60 << 20),
        cost_estimate=pl.CostEstimate(flops=16 * width * rank * rows, bytes_accessed=20 << 20, transcendentals=rows),
        name="step",
    )(
        slot_of_block,
        received,
        dense_part,
        row_data,
        col_data,
        jnp.swapaxes(proj_wide, 1, 2),
        jnp.swapaxes(proj_mid, 1, 2),
        jnp.swapaxes(proj_narrow, 1, 2),
        proj_wide,
        proj_mid,
        proj_narrow,
        jnp.swapaxes(cross_in, 1, 2),
        cross_in,
        jnp.swapaxes(cross_out, 1, 2),
        cross_out,
    )
    back = back.reshape(devices, blocks_here * BLOCK_WIDTH, rows)
    back = lax.all_to_all(back, AXES, 0, 0, tiled=True)

    cut = splits[0] - rank
    fixed = (devices, chunk, chunk_pad)
    los, his = weight_grads(
        me, small, (low1, layer1, low0, start),
        [[(0, 1, 0, rank), (1, 2, 0, cut)], [(1, 2, cut, rank), (2, 0, 0, rank)], [(3, 3, 0, rank)]],
        [0, 2, None], orders, *fixed,
    )
    mine, got = reduce_pieces(los, his, orders, devices)
    grad_in, grad_out, grad_bias = finish(mine, got, rank, chunk)
    grad_in = jnp.transpose(grad_in, (1, 0, 2))
    grad_out = jnp.transpose(grad_out, (1, 2, 0))
    pooled_grad = unpack(back)
    return (pooled_grad, grad_in, grad_out, grad_bias)


def solution(mesh):
    return jax.shard_map(
        run,
        mesh=mesh,
        in_specs=(
            P(None, AXES, None),
            P(),
            P(None, AXES),
            P(AXES),
            P(AXES),
            P(),
            P(),
            P(),
            P(),
            P(),
            P(),
            P(),
        ),
        out_specs=(
            P(None, AXES, None),
            P(None, AXES, None),
            P(None, None, AXES),
            P(None, AXES),
        ),
        check_vma=False,
    )
```
